32 devices in a mesh: dp: 8 (over z, x), tensor: 4 (over y, core).
Axes of the slice: x: 2, y: 2, z: 4, core: 2. Of those that a mesh axis runs over, the one named last changes fastest.
Arguments:
- tokens: bfloat16 [16384, 768], P(('dp', 'tensor')), may hold values from -6 to 6
- lengths: int32 [32], P('dp'), may hold values from 128 to 512, as said below
- w_query: bfloat16 [768, 768], P(None, 'tensor'), may hold values from -0.3125 to 0.3125
- b_query: bfloat16 [768], P('tensor'), may hold values from -4 to 4
- w_key: bfloat16 [768, 768], P(None, 'tensor'), may hold values from -0.3125 to 0.3125
- w_value: bfloat16 [768, 768], P(None, 'tensor'), may hold values from -0.21875 to 0.21875
- b_value: bfloat16 [768], P('tensor'), may hold values from -4 to 4
- w_out: bfloat16 [768, 768], P('tensor'), may hold values from -1.25 to 1.25
- b_out: bfloat16 [768], replicated, may hold values from -4 to 4
- gain_one: bfloat16 [768], replicated, may hold values from 0.25 to 1.75
- shift_one: bfloat16 [768], replicated, may hold values from -4 to 4
- w_up: bfloat16 [768, 3072], P(None, 'tensor'), may hold values from -0.21875 to 0.21875
- b_up: bfloat16 [3072], P('tensor'), may hold values from -4 to 4
- w_down: bfloat16 [3072, 768], P('tensor'), may hold values from -0.109375 to 0.109375
- b_down: bfloat16 [768], replicated, may hold values from -4 to 4
- gain_two: bfloat16 [768], replicated, may hold values from 0.25 to 1.75
- shift_two: bfloat16 [768], replicated, may hold values from -4 to 4
- cotangent: bfloat16 [16384, 768], P(('dp', 'tensor')), may hold values from -6 to 6
Outputs:
- result: bfloat16 [16384, 768], P(('dp', 'tensor'))
- grad_tokens: float32 [16384, 768], P(('dp', 'tensor'))
- grad_w_query: float32 [768, 768], P(None, 'tensor')
- grad_b_query: float32 [768], P('tensor')
- grad_w_key: float32 [768, 768], P(None, 'tensor')
- grad_w_value: float32 [768, 768], P(None, 'tensor')
- grad_b_value: float32 [768], P('tensor')
- grad_w_out: float32 [768, 768], P('tensor')
- grad_b_out: float32 [768], replicated
- grad_gain_one: float32 [768], replicated
- grad_shift_one: float32 [768], replicated
- grad_w_up: float32 [768, 3072], P(None, 'tensor')
- grad_b_up: float32 [3072], P('tensor')
- grad_w_down: float32 [3072, 768], P('tensor')
- grad_b_down: float32 [768], replicated
- grad_gain_two: float32 [768], replicated
- grad_shift_two: float32 [768], replicated
The draws below stay inside these ranges and needn't reach their ends.
Inputs may be any that keep to these rules, and one draw needn't show every extreme that they name: `lengths`: valid leading tokens of each sequence; in every draw some sequence is full and some holds exactly 128.
All inputs are finite; a program needn't handle non-finite values.
Results may differ from the reference program's by a relative error of at most 0.015.
The reference program's roundings to bfloat16 on the way count: a program that leaves them out, or rounds other values in their place, can miss the bound.
Values may be sent and summed in bfloat16 or wider, within the bound.
A program may use at most 128 MiB of HBM per device.

```python
import jax
import jax.numpy as jnp
from jax import lax

D = 768
HEADS = 12
HEAD_DIM = 64
FF = 3072
SEQ_LEN = 512
SEQ_DEV = 4
TOK_DEV = 2048
SEQS = 32
TOKENS = 16384
N_DP = 8


def draw_lengths(key, part):
    first, second, third = jax.random.split(key, 3)
    values = jax.random.randint(first, (SEQS,), SEQ_LEN // 4, SEQ_LEN + 1)
    full_at = jax.random.randint(second, (), 0, SEQS)
    least_at = (full_at + 1 + jax.random.randint(third, (), 0, SEQS - 1)) % SEQS
    values = values.at[full_at].set(SEQ_LEN)
    values = values.at[least_at].set(SEQ_LEN // 4)
    return values.astype(jnp.int32)


def block_levels(stream_key, shape, shards, smallest, high):
    def one(position, blocks):
        draws = jax.random.uniform(jax.random.fold_in(jax.random.fold_in(stream_key, 6), position), (blocks,), jnp.float32, smallest / len(shards), high / len(shards))
        return jnp.repeat(jnp.exp(draws), shape[position] // blocks).reshape((-1,) + (1,) * (len(shape) - position - 1))

    loudness = one(*shards[0])
    for cut in shards[1:]:
        loudness = loudness * one(*cut)
    return loudness


def gaussian(own_key, extent, deviation, bound, pieces=(), held_as=jnp.bfloat16):
    level = block_levels(own_key, extent, pieces, -0.22, 0.18) if pieces else 1.0
    values = jax.random.normal(own_key, extent, jnp.float32) * deviation * level
    return jnp.minimum(jnp.maximum(values, -bound), bound).astype(held_as)


def setup_inputs(seed: int = 0) -> dict:
    splits = jax.random.split(jax.random.key(seed), 19)
    return {
        "tokens": gaussian(splits[0], (TOKENS, D), 1.0, 6.0, ((0, 32),)),
        "lengths": draw_lengths(jax.random.fold_in(splits[18], 71), 0),
        "w_query": gaussian(splits[2], (D, D), (D // 2) ** -0.5, 0.3125, ((1, 4),)),
        "b_query": gaussian(splits[3], (D,), 0.3, 4.0, ((0, 4),)),
        "w_key": gaussian(splits[4], (D, D), (D // 2) ** -0.5, 0.3125, ((1, 4),)),
        "w_value": gaussian(splits[5], (D, D), D ** -0.5, 0.21875, ((1, 4),)),
        "b_value": gaussian(splits[6], (D,), 0.3, 4.0, ((0, 4),)),
        "w_out": gaussian(splits[7], (D, D), (D // 32) ** -0.5, 1.25, ((0, 4),)),
        "b_out": gaussian(splits[8], (D,), 0.3, 4.0),
        "gain_one": jnp.clip(1.0 + 0.15 * jax.random.normal(splits[9], (D,), jnp.float32), 0.25, 1.75).astype(jnp.bfloat16),
        "shift_one": gaussian(splits[10], (D,), 0.3, 4.0),
        "w_up": gaussian(splits[11], (D, FF), D ** -0.5, 0.21875, ((1, 4),)),
        "b_up": gaussian(splits[12], (FF,), 0.3, 4.0, ((0, 4),)),
        "w_down": gaussian(splits[13], (FF, D), FF ** -0.5, 0.109375, ((0, 4),)),
        "b_down": gaussian(splits[14], (D,), 0.3, 4.0),
        "gain_two": jnp.clip(1.0 + 0.15 * jax.random.normal(splits[15], (D,), jnp.float32), 0.25, 1.75).astype(jnp.bfloat16),
        "shift_two": gaussian(splits[16], (D,), 0.3, 4.0),
        "cotangent": gaussian(splits[17], (TOKENS, D), 1.0, 6.0, ((0, 32),)),
    }


@jax.custom_vjp
def low(v):
    return lax.optimization_barrier(v.astype(jnp.bfloat16)).astype(jnp.float32)

@jax.custom_vjp
def low_back(v):
    return v

def low_keep(v):
    return (low(v), None)

def low_pass(kept, grad):
    return (grad,)

def back_keep(v):
    return (v, None)

def back_low(kept, grad):
    return (low(grad),)
low.defvjp(low_keep, low_pass)
low_back.defvjp(back_keep, back_low)
EPSILON = 1e-12

def rounded(value):
    return low(low_back(value))

def matmul(left, right):
    return jnp.dot(left, right, precision=lax.Precision.HIGHEST)

def layer_norm(value, gain, shift):
    centre = value - lax.optimization_barrier(jnp.mean(value, -1, keepdims=True))
    inverse = lax.rsqrt(lax.optimization_barrier(jnp.mean(centre * centre, -1, keepdims=True)) + EPSILON)
    return centre * inverse * gain + shift

def attend(item):
    queries, key_rows, value_rows, length = item
    scores = low_back(jnp.einsum('qhd,khd->hqk', queries, key_rows, precision=lax.Precision.HIGHEST))
    scores = scores * HEAD_DIM ** (-0.5)
    key_valid = jnp.arange(queries.shape[0])[None, None, :] < length
    scores = jnp.where(key_valid, scores, -1e+30)
    probs = jax.nn.softmax(scores, -1)
    return jnp.einsum('hqk,khd->qhd', low(probs), value_rows, precision=lax.Precision.HIGHEST)

def forward(rows, counts, params):
    w_query, b_query, w_key, w_value, b_value, w_out, b_out, gain_one, shift_one, w_up, b_up, w_down, b_down, gain_two, shift_two = params
    seqs_here = counts.shape[0]
    shape_heads = (seqs_here, SEQ_LEN, HEADS, HEAD_DIM)
    queries = rounded(matmul(rows, w_query) + b_query).reshape(shape_heads)
    key_rows = rounded(matmul(rows, w_key)).reshape(shape_heads)
    value_rows = rounded(matmul(rows, w_value) + b_value).reshape(shape_heads)
    context = lax.map(jax.checkpoint(attend), (queries, key_rows, value_rows, counts))
    context = rounded(context.reshape(rows.shape[0], D))
    attn_out = low_back(matmul(context, w_out))
    normed_one = layer_norm(rows + attn_out + b_out, gain_one, shift_one)
    pre_act = low_back(matmul(low(normed_one), w_up) + b_up)
    activ = low(jax.nn.gelu(pre_act, approximate=False))
    ffn_out = low_back(matmul(activ, w_down))
    return layer_norm(normed_one + ffn_out + b_down, gain_two, shift_two)

def reference(tokens, lengths, w_query, b_query, w_key, w_value, b_value, w_out, b_out, gain_one, shift_one, w_up, b_up, w_down, b_down, gain_two, shift_two, cotangent):
    params = tuple((p.astype(jnp.float32) for p in (w_query, b_query, w_key, w_value, b_value, w_out, b_out, gain_one, shift_one, w_up, b_up, w_down, b_down, gain_two, shift_two)))
    rows_all = tokens.astype(jnp.float32).reshape(N_DP, TOK_DEV, D)
    counts_all = lengths.reshape(N_DP, SEQ_DEV)
    grads_all = cotangent.astype(jnp.float32).reshape(N_DP, TOK_DEV, D)

    def group(carry, item):
        rows, counts, incoming = item
        valid = (jnp.arange(SEQ_LEN)[None, :] < counts[:, None]).reshape(TOK_DEV, 1).astype(jnp.float32)
        output, pull = jax.vjp(lambda r, p: forward(r, counts, p), rows, params)
        d_rows, d_params = pull(incoming * valid)
        return (tuple((c + g for c, g in zip(carry, d_params))), (output.astype(jnp.bfloat16), d_rows))
    start = tuple((jnp.zeros_like(p) for p in params))
    sums, (outputs, d_rows) = lax.scan(group, start, (rows_all, counts_all, grads_all))
    return (outputs.reshape(TOKENS, D), d_rows.reshape(TOKENS, D), sums[0], sums[1], sums[2], sums[3], sums[4], sums[5], sums[6], sums[7], sums[8], sums[9], sums[10], sums[11], sums[12], sums[13], sums[14])
```

```python
import functools

import jax
import jax.numpy as jnp
from jax import lax
from jax.experimental import pallas as pl
from jax.experimental.pallas import tpu as pltpu
from jax.sharding import PartitionSpec as P

HEAD_DIM = 64
SEQ_LEN = 512
EPSILON = 1e-12
F32 = jnp.float32
BF16 = jnp.bfloat16


def swap(value, axis, bit):
    size = lax.axis_size(axis)
    return lax.ppermute(value, axis, [(i, i ^ bit) for i in range(size)])


def bits_of(size):
    bit, found = 1, []
    while bit < size:
        found.append(bit)
        bit *= 2
    return found


def gather_blocks(own, axis):
    size = lax.axis_size(axis)
    blocks = [own]
    for r in range(1, size):
        low = r & -r
        blocks.append(swap(blocks[r ^ low], axis, low))
    return blocks


def partner_of(index, bit):
    return index + bit - 2 * bit * ((index // bit) % 2)


def add_rows(target, start, source, count, result=None):
    tile = 48
    result = target if result is None else result

    def step(i, carry):
        here = pl.ds(pl.multiple_of(start + i * tile, 16), tile)
        there = pl.ds(pl.multiple_of(i * tile, 16), tile)
        result[here, :] = (target[here, :].astype(F32) + source[there, :].astype(F32)).astype(BF16)
        return carry

    lax.fori_loop(0, count // tile, step, 0)


def halvings(count, groups):
    plan = []
    for bit in bits_of(groups):
        halves = (count // 2) % 48 == 0
        count = count // 2 if halves else count
        plan.append((bit, count, halves))
    return plan


class Chunk:
    def __init__(self, blocks, near, far, full, arrived, place, sems, groups):
        self.blocks, self.near, self.far, self.full, self.arrived = blocks, near, far, full, arrived
        self.place, self.sems = place, sems
        self.rows = near.shape[0]
        self.plan = halvings(self.rows, groups)
        self.count, self.start = self.rows, 0
        self.pending, self.slot = [], 0

    def send(self, source, target, where):
        send_sem, recv_sem = self.sems
        copy = pltpu.make_async_remote_copy(
            src_ref=source, dst_ref=target, send_sem=send_sem.at[self.slot], recv_sem=recv_sem.at[self.slot],
            device_id=where, device_id_type=pl.DeviceIdType.MESH,
        )
        self.slot += 1
        copy.start()
        return copy

    def pair_start(self):
        other = {"tensor": partner_of(self.place[1], 1)}
        self.to_far = self.send(self.blocks[3], self.far, other)
        self.to_near = self.send(self.blocks[1], self.near, other)

    def pair_finish(self):
        self.to_far.wait()
        add_rows(self.far, 0, self.blocks[2], self.rows)
        self.to_near.wait()
        add_rows(self.near, 0, self.blocks[0], self.rows)
        self.pending = [self.send(self.far, self.arrived[0], {"tensor": partner_of(self.place[1], 2)})]

    def window(self, start, count):
        return pl.ds(pl.multiple_of(start, 16), count)

    def finish(self, stage):
        for copy in self.pending:
            copy.wait()
        bits = len(self.plan)
        if stage <= bits:
            result = self.full if stage == bits else None
            add_rows(self.near, self.start, self.arrived[stage], self.count, result)

    def begin(self, stage):
        bits = len(self.plan)
        if stage < bits:
            bit, count, halves = self.plan[stage]
            other = {"dp": partner_of(self.place[0], bit)}
            mine = (self.place[0] // bit) % 2
            if halves:
                sent = self.start + (1 - mine) * count
                self.start = self.start + mine * count
                self.count = count
            else:
                sent = self.start
            source = self.near.at[self.window(sent, count), :]
            self.pending = [self.send(source, self.arrived[stage + 1], other)]
        elif stage < 2 * bits:
            bit, count, halves = self.plan[2 * bits - 1 - stage]
            self.pending = []
            if halves:
                mine = (self.place[0] // bit) % 2
                here = self.full.at[self.window(self.start, count), :]
                self.pending = [self.send(here, here, {"dp": partner_of(self.place[0], bit)})]
                self.start = self.start - mine * count
                self.count = 2 * count


class Vectors:
    def __init__(self, values, sums, arrived, place, sems, ways, groups):
        self.values, self.sums, self.arrived, self.place, self.sems = values, sums, arrived, place, sems
        self.ways = ways
        self.steps = [("tensor", b) for b in bits_of(ways)] + [("dp", b) for b in bits_of(groups)]

    def begin(self, step):
        axis, bit = self.steps[step]
        index = self.place[1] if axis == "tensor" else self.place[0]
        source = self.values if step == 0 else self.sums.at[step - 1]
        self.copy = pltpu.make_async_remote_copy(
            src_ref=source, dst_ref=self.arrived.at[step], send_sem=self.sems[0].at[step],
            recv_sem=self.sems[1].at[step], device_id={axis: partner_of(index, bit)},
            device_id_type=pl.DeviceIdType.MESH,
        )
        self.copy.start()

    def finish(self, step):
        self.copy.wait()
        axis, bit = self.steps[step]
        source = self.values if step == 0 else self.sums.at[step - 1]
        for r in range(self.ways + 1):
            swapped = r ^ bit if axis == "tensor" and r < self.ways else r
            self.sums[step, 8 * r : 8 * r + 8, :] = (
                source[8 * r : 8 * r + 8, :] + self.arrived[step, 8 * swapped : 8 * swapped + 8, :]
            )


def reduce_kernel(ways, groups, cuts, counts, *refs):
    weights = len(cuts)
    blocks = [refs[w * ways : (w + 1) * ways] for w in range(weights)]
    refs = refs[weights * ways :]
    small, refs = refs[0], refs[1:]
    outs, small_out, refs = refs[:weights], refs[weights], refs[weights + 1 :]
    small_sums, small_arrived, small_send, small_recv, chunk_send, chunk_recv = refs[:6]
    refs = refs[6:]
    place = (lax.axis_index("dp"), lax.axis_index("tensor"))

    barrier = pltpu.get_barrier_semaphore()
    partners = [{"tensor": partner_of(place[1], b)} for b in bits_of(ways)]
    partners += [{"dp": partner_of(place[0], b)} for b in bits_of(groups)]
    for partner in partners:
        pl.semaphore_signal(barrier, inc=1, device_id=partner, device_id_type=pl.DeviceIdType.MESH)
    pl.semaphore_wait(barrier, len(partners))

    vectors = Vectors(small, small_sums, small_arrived, place, (small_send, small_recv), ways, groups)
    bits = len(bits_of(groups))
    chunks, finals, used = [], [], 0
    for w, cut in enumerate(cuts):
        rows = counts[w] // cut
        for c in range(cut):
            own = [block.at[c * rows : (c + 1) * rows, :] for block in blocks[w]]
            near, far, full, *arrived = refs[used : used + 4 + bits]
            used += 4 + bits
            number = len(chunks)
            chunks.append(
                Chunk(own, near, far, full, arrived, place, (chunk_send.at[number], chunk_recv.at[number]), groups)
            )
            finals.append((outs[w], c * rows, rows))

    for chunk in chunks:
        chunk.pair_start()
    vectors.begin(0)
    for chunk in chunks:
        chunk.pair_finish()
    last = 2 * bits
    steps = len(vectors.steps)
    for wave in range(len(chunks) + last):
        live = [(n, wave - n) for n in range(len(chunks)) if 0 <= wave - n <= last]
        for n, stage in live:
            chunks[n].finish(stage)
            if stage < last:
                chunks[n].begin(stage)
            else:
                out, start, rows = finals[n]
                out[start : start + rows, :] = chunks[n].full[...]
        if wave < steps:
            vectors.finish(wave)
            if wave + 1 < steps:
                vectors.begin(wave + 1)
    small_out[...] = small_sums[steps - 1]


def reduce_gradients(gradients, cuts, small):
    ways, groups = lax.axis_size("tensor"), lax.axis_size("dp")
    bits = len(bits_of(groups))
    steps = bits + len(bits_of(ways))
    counts = [g[0].shape[0] for g in gradients]
    shape = jax.ShapeDtypeStruct
    scratch = [
        pltpu.VMEM((steps,) + small.shape, F32),
        pltpu.VMEM((steps,) + small.shape, F32),
        pltpu.SemaphoreType.DMA((steps,)),
        pltpu.SemaphoreType.DMA((steps,)),
        pltpu.SemaphoreType.DMA((sum(cuts), 3 + 2 * bits)),
        pltpu.SemaphoreType.DMA((sum(cuts), 3 + 2 * bits)),
    ]
    for g, cut in zip(gradients, cuts):
        rows, cols = g[0].shape
        for _ in range(cut):
            scratch += [pltpu.VMEM((rows // cut, cols), BF16)] * 4
            scratch += [pltpu.VMEM((count, cols), BF16) for _, count, _ in halvings(rows // cut, groups)]
    flat = [block for g in gradients for block in g]
    outs = pl.pallas_call(
        functools.partial(reduce_kernel, ways, groups, cuts, counts),
        out_shape=[shape(g[0].shape, BF16) for g in gradients] + [shape(small.shape, F32)],
        in_specs=[VMEM_SPEC] * (len(flat) + 1),
        out_specs=[VMEM_SPEC] * (len(gradients) + 1),
        scratch_shapes=scratch,
        compiler_params=pltpu.CompilerParams(
            collective_id=0, has_side_effects=True, vmem_limit_bytes=56 * 2**20
        ),
        name="reduce_gradients",
    )(*flat, small)
    return [o.astype(F32) for o in outs[:-1]], outs[-1]


def dot(left, right, dims):
    return lax.dot_general(left, right, (dims, ((), ())), preferred_element_type=F32)


NN = ((1,), (0,))
NT = ((1,), (1,))
TN = ((0,), (0,))


def attend_forward_kernel(
    length_ref, rows_ref, wq_ref, wk_ref, wv_ref, bq_ref, bv_ref,
    q_ref, k_ref, v_ref, context_ref, context_t_ref, log_ref,
):
    length = length_ref[0]
    rows = rows_ref[...]
    q_ref[...] = (jnp.dot(rows, wq_ref[...], preferred_element_type=F32) + bq_ref[...]).astype(BF16)
    k_ref[...] = jnp.dot(rows, wk_ref[...], preferred_element_type=F32).astype(BF16)
    v_ref[...] = (jnp.dot(rows, wv_ref[...], preferred_element_type=F32) + bv_ref[...]).astype(BF16)
    size = rows.shape[0]
    key_valid = lax.broadcasted_iota(jnp.int32, (size, size), 0) < length
    for head in range(q_ref.shape[1] // HEAD_DIM):
        part = slice(head * HEAD_DIM, (head + 1) * HEAD_DIM)
        scaled = (q_ref[:, part].astype(F32) * HEAD_DIM ** (-0.5)).astype(BF16)
        scores = dot(k_ref[:, part], scaled, NT)
        scores = jnp.where(key_valid, scores, -1e30)
        highest = jnp.max(scores, 0, keepdims=True)
        expo = jnp.exp(scores - highest)
        totals = jnp.sum(expo, 0, keepdims=True)
        probs_low = (expo * (1.0 / totals)).astype(BF16)
        context_t = dot(v_ref[:, part], probs_low, TN)
        context_t_ref[part, :] = context_t.astype(BF16)
        context_ref[:, part] = context_t.T.astype(BF16)
        log_ref[head : head + 1, :] = highest + jnp.log(totals)


def attend_backward_kernel(
    length_ref, q_ref, k_ref, v_ref, log_ref, d_rows_ref, wo_ref,
    dq_ref, dk_ref, dv_ref, d_context_ref,
):
    length = length_ref[0]
    d_context_ref[...] = dot(d_rows_ref[...], wo_ref[...], NT).astype(BF16)
    size = q_ref.shape[0]
    key_valid = lax.broadcasted_iota(jnp.int32, (size, size), 0) < length
    for head in range(q_ref.shape[1] // HEAD_DIM):
        part = slice(head * HEAD_DIM, (head + 1) * HEAD_DIM)
        scaled = (q_ref[:, part].astype(F32) * HEAD_DIM ** (-0.5)).astype(BF16)
        keys = k_ref[:, part]
        d_context = d_context_ref[:, part]
        scores = dot(keys, scaled, NT)
        scores = jnp.where(key_valid, scores, -1e30)
        probs = jnp.exp(scores - log_ref[head : head + 1, :])
        d_probs = dot(v_ref[:, part], d_context, NT)
        dv_ref[:, part] = jnp.dot(probs.astype(BF16), d_context, preferred_element_type=F32).astype(BF16)
        centre = jnp.sum(probs * d_probs, 0, keepdims=True)
        d_scores = (probs * (d_probs - centre)).astype(BF16)
        dk_ref[:, part] = jnp.dot(d_scores, scaled, preferred_element_type=F32).astype(BF16)
        d_query_t = dot(keys, d_scores, TN) * HEAD_DIM ** (-0.5)
        dq_ref[:, part] = d_query_t.T.astype(BF16)


VMEM_SPEC = pl.BlockSpec(memory_space=pltpu.VMEM)
SMEM_SPEC = pl.BlockSpec(memory_space=pltpu.SMEM)


def attend_forward(length, rows, wq, wk, wv, bq, bv):
    count, cols = rows.shape[0], wq.shape[1]
    shape = jax.ShapeDtypeStruct
    heads = cols // HEAD_DIM
    return pl.pallas_call(
        attend_forward_kernel,
        out_shape=[shape((count, cols), BF16)] * 4 + [shape((cols, count), BF16), shape((heads, count), F32)],
        in_specs=[SMEM_SPEC] + [VMEM_SPEC] * 6,
        out_specs=[VMEM_SPEC] * 6,
        cost_estimate=pl.CostEstimate(
            flops=2 * count * (3 * rows.shape[1] * cols + 2 * count * cols),
            bytes_accessed=2 * (rows.size + 3 * wq.size + 5 * count * cols),
            transcendentals=count * count * heads,
        ),
        compiler_params=pltpu.CompilerParams(vmem_limit_bytes=32 * 2**20),
        name="attend_forward",
    )(length, rows, wq, wk, wv, bq, bv)


def attend_backward(length, q, k, v, log_total, d_rows, w_out):
    count, cols = q.shape
    shape = jax.ShapeDtypeStruct
    return pl.pallas_call(
        attend_backward_kernel,
        out_shape=[shape((count, cols), BF16)] * 3,
        in_specs=[SMEM_SPEC] + [VMEM_SPEC] * 6,
        out_specs=[VMEM_SPEC] * 3,
        scratch_shapes=[pltpu.VMEM((count, cols), BF16)],
        cost_estimate=pl.CostEstimate(
            flops=2 * count * (w_out.size + 5 * count * cols),
            bytes_accessed=2 * (d_rows.size + w_out.size + 6 * count * cols),
            transcendentals=count * count * (cols // HEAD_DIM),
        ),
        compiler_params=pltpu.CompilerParams(vmem_limit_bytes=32 * 2**20),
        name="attend_backward",
    )(length, q, k, v, log_total, d_rows, w_out)


def normalise(value):
    centre = value - jnp.mean(value, -1, keepdims=True)
    inverse = lax.rsqrt(jnp.mean(centre * centre, -1, keepdims=True) + EPSILON)
    return centre * inverse, inverse


def norm_back(incoming, normal, inverse, gain):
    d_gain = jnp.sum(incoming * normal, 0)
    d_shift = jnp.sum(incoming, 0)
    scaled = incoming * gain
    d_input = inverse * (
        scaled
        - jnp.mean(scaled, -1, keepdims=True)
        - normal * jnp.mean(scaled * normal, -1, keepdims=True)
    )
    return d_input, d_gain, d_shift


def local(
    tokens, lengths, w_query, b_query, w_key, w_value, b_value, w_out, b_out,
    gain_one, shift_one, w_up, b_up, w_down, b_down, gain_two, shift_two, cotangent,
):
    own_rows, width = tokens.shape
    ways = lax.axis_size("tensor")
    me = lax.axis_index("tensor")
    local_cols = w_query.shape[1]
    length = lax.dynamic_slice(lengths, (me,), (1,))
    gain_a, shift_a = gain_one.astype(F32), shift_one.astype(F32)
    gain_b, shift_b = gain_two.astype(F32), shift_two.astype(F32)

    biases = jnp.concatenate([b_query, b_value, b_up]).reshape(1, -1).astype(F32)
    biases = gather_blocks(biases, "tensor")
    b_query_all = [b[:, :local_cols] for b in biases]
    b_value_all = [b[:, local_cols : 2 * local_cols] for b in biases]
    b_up_all = [b[:, 2 * local_cols :] for b in biases]
    wq_all = gather_blocks(w_query, "tensor")
    wk_all = gather_blocks(w_key, "tensor")
    wv_all = gather_blocks(w_value, "tensor")
    wo_all = gather_blocks(w_out, "tensor")
    up_all = gather_blocks(w_up, "tensor")
    down_all = gather_blocks(w_down, "tensor")

    saved, attn_out = [], 0.0
    for r in range(ways):
        q, k, v, context, context_t, log_total = attend_forward(
            length, tokens, wq_all[r], wk_all[r], wv_all[r], b_query_all[r], b_value_all[r]
        )
        saved.append((q, k, v, context_t, log_total))
        attn_out = attn_out + dot(context, wo_all[r], NN)
    resid_one = tokens.astype(F32) + attn_out + b_out.astype(F32)
    unit_one, inverse_one = normalise(resid_one)
    normed_one = unit_one * gain_a + shift_a
    normed_low = normed_one.astype(BF16)

    ffn_out, acts, slopes = 0.0, [], []
    for r in range(ways):
        pre_act = dot(normed_low, up_all[r], NN) + b_up_all[r]
        share = 0.5 * (1.0 + lax.erf(pre_act * 0.5**0.5))
        activ = (pre_act * share).astype(BF16)
        slope = share + pre_act * jnp.exp(-0.5 * pre_act * pre_act) * (2.0 * jnp.pi) ** (-0.5)
        acts.append(activ)
        slopes.append(slope)
        ffn_out = ffn_out + dot(activ, down_all[r], NN)
    unit_two, inverse_two = normalise(normed_one + ffn_out + b_down.astype(F32))
    result = (unit_two * gain_b + shift_b).astype(BF16)

    row_valid = (jnp.arange(own_rows) < length[0]).astype(F32)[:, None]
    incoming = cotangent.astype(F32) * row_valid
    d_two, d_gain_two, d_shift_two = norm_back(incoming, unit_two, inverse_two, gain_b)
    d_b_down = jnp.sum(d_two, 0)
    d_two_low = d_two.astype(BF16)
    d_one_out = d_two
    d_down, d_up, d_b_up = [None] * ways, [None] * ways, [None] * ways
    for r in reversed(range(ways)):
        d_down[r] = dot(acts[r], d_two_low, TN).astype(BF16)
        d_pre = (dot(d_two_low, down_all[r], NT) * slopes[r]).astype(BF16)
        d_up[r] = dot(normed_low, d_pre, TN).astype(BF16)
        d_b_up[r] = jnp.sum(d_pre.astype(F32), 0)
        d_one_out = d_one_out + dot(d_pre, up_all[r], NT)

    d_one, d_gain_one, d_shift_one = norm_back(d_one_out, unit_one, inverse_one, gain_a)
    d_b_out = jnp.sum(d_one, 0)
    d_one_low = d_one.astype(BF16)
    d_out = [dot(saved[r][3], d_one_low, NN).astype(BF16) for r in range(ways)]

    grad_tokens = d_one
    d_joint, d_bias = [None] * ways, [None] * ways
    for r in reversed(range(ways)):
        q, k, v, _, log_total = saved[r]
        dq, dk, dv = attend_backward(length, q, k, v, log_total, d_one_low, wo_all[r])
        d_joint[r] = jnp.concatenate(
            [dot(tokens, part, TN).astype(BF16) for part in (dq, dk, dv)], 1
        )
        d_bias[r] = jnp.stack([jnp.sum(dq.astype(F32), 0), jnp.sum(dv.astype(F32), 0)])
        grad_tokens = grad_tokens + dot(dq, wq_all[r], NT) + dot(dk, wk_all[r], NT) + dot(dv, wv_all[r], NT)
    parts = []
    for r in range(ways):
        pair = jnp.concatenate([d_bias[r].reshape(-1), jnp.zeros((width - 2 * local_cols,), F32)])
        parts += [d_b_up[r], pair] + [jnp.zeros((width,), F32)] * 6
    parts += [d_gain_one, d_shift_one, d_b_out, d_b_down, d_gain_two, d_shift_two] + [jnp.zeros((width,), F32)] * 2
    sums, small = reduce_gradients([d_down, d_up, d_out, d_joint], (2, 2, 1, 2), jnp.stack(parts))
    grad_w_down, grad_w_up, grad_w_out, d_w_joint = sums
    shared = small[8 * ways :]

    return (
        result,
        grad_tokens,
        d_w_joint[:, :local_cols],
        small[1, :local_cols],
        d_w_joint[:, local_cols : 2 * local_cols],
        d_w_joint[:, 2 * local_cols :],
        small[1, local_cols : 2 * local_cols],
        grad_w_out,
        shared[2],
        shared[0],
        shared[1],
        grad_w_up,
        small[0],
        grad_w_down,
        shared[3],
        shared[4],
        shared[5],
    )


def solution(mesh):
    rows = P(("dp", "tensor"), None)
    in_specs = (
        rows, P("dp"), P(None, "tensor"), P("tensor"), P(None, "tensor"), P(None, "tensor"), P("tensor"),
        P("tensor", None), P(), P(), P(), P(None, "tensor"), P("tensor"), P("tensor", None), P(), P(), P(), rows,
    )
    out_specs = (
        rows, rows, P(None, "tensor"), P("tensor"), P(None, "tensor"), P(None, "tensor"), P("tensor"),
        P("tensor", None), P(), P(), P(), P(None, "tensor"), P("tensor"), P("tensor", None), P(), P(), P(),
    )
    return jax.shard_map(local, mesh=mesh, in_specs=in_specs, out_specs=out_specs, check_vma=False)
```

```python
import functools

import jax
import jax.numpy as jnp
from jax import lax
from jax.experimental import pallas as pl
from jax.experimental.pallas import tpu as pltpu
from jax.sharding import PartitionSpec as P

HEAD_DIM = 64
SEQ_LEN = 512
EPSILON = 1e-12
F32 = jnp.float32
BF16 = jnp.bfloat16


def swap(value, axis, bit):
    size = lax.axis_size(axis)
    return lax.ppermute(value, axis, [(i, i ^ bit) for i in range(size)])


def bits_of(size):
    bit, found = 1, []
    while bit < size:
        found.append(bit)
        bit *= 2
    return found


def gather_blocks(own, axis):
    size = lax.axis_size(axis)
    blocks = [own]
    for r in range(1, size):
        low = r & -r
        blocks.append(swap(blocks[r ^ low], axis, low))
    return blocks


def partner_of(index, bit):
    return index + bit - 2 * bit * ((index // bit) % 2)


def add_rows(target, start, source, count, result=None):
    tile = 48
    result = target if result is None else result

    def step(i, carry):
        here = pl.ds(pl.multiple_of(start + i * tile, 16), tile)
        there = pl.ds(pl.multiple_of(i * tile, 16), tile)
        result[here, :] = (target[here, :].astype(F32) + source[there, :].astype(F32)).astype(BF16)
        return carry

    lax.fori_loop(0, count // tile, step, 0)


def halvings(count, groups):
    plan = []
    for bit in bits_of(groups):
        halves = (count // 2) % 48 == 0
        count = count // 2 if halves else count
        plan.append((bit, count, halves))
    return plan


class Chunk:
    def __init__(self, blocks, near, far, full, arrived, place, sems, groups):
        self.blocks, self.near, self.far, self.full, self.arrived = blocks, near, far, full, arrived
        self.place, self.sems = place, sems
        self.rows = near.shape[0]
        self.plan = halvings(self.rows, groups)
        self.count, self.start = self.rows, 0
        self.pending, self.slot = [], 0

    def send(self, source, target, where):
        send_sem, recv_sem = self.sems
        copy = pltpu.make_async_remote_copy(
            src_ref=source, dst_ref=target, send_sem=send_sem.at[self.slot], recv_sem=recv_sem.at[self.slot],
            device_id=where, device_id_type=pl.DeviceIdType.MESH,
        )
        self.slot += 1
        copy.start()
        return copy

    def pair_start(self):
        other = {"tensor": partner_of(self.place[1], 1)}
        self.to_far = self.send(self.blocks[3], self.far, other)
        self.to_near = self.send(self.blocks[1], self.near, other)

    def pair_finish(self):
        self.to_far.wait()
        add_rows(self.far, 0, self.blocks[2], self.rows)
        self.to_near.wait()
        add_rows(self.near, 0, self.blocks[0], self.rows)
        self.pending = [self.send(self.far, self.arrived[0], {"tensor": partner_of(self.place[1], 2)})]

    def window(self, start, count):
        return pl.ds(pl.multiple_of(start, 16), count)

    def finish(self, stage):
        for copy in self.pending:
            copy.wait()
        bits = len(self.plan)
        if stage <= bits:
            result = self.full if stage == bits else None
            add_rows(self.near, self.start, self.arrived[stage], self.count, result)

    def begin(self, stage):
        bits = len(self.plan)
        if stage < bits:
            bit, count, halves = self.plan[stage]
            other = {"dp": partner_of(self.place[0], bit)}
            mine = (self.place[0] // bit) % 2
            if halves:
                sent = self.start + (1 - mine) * count
                self.start = self.start + mine * count
                self.count = count
            else:
                sent = self.start
            source = self.near.at[self.window(sent, count), :]
            self.pending = [self.send(source, self.arrived[stage + 1], other)]
        elif stage < 2 * bits:
            bit, count, halves = self.plan[2 * bits - 1 - stage]
            self.pending = []
            if halves:
                mine = (self.place[0] // bit) % 2
                here = self.full.at[self.window(self.start, count), :]
                self.pending = [self.send(here, here, {"dp": partner_of(self.place[0], bit)})]
                self.start = self.start - mine * count
                self.count = 2 * count


class Vectors:
    def __init__(self, values, sums, arrived, place, sems, ways, groups):
        self.values, self.sums, self.arrived, self.place, self.sems = values, sums, arrived, place, sems
        self.ways = ways
        self.steps = [("tensor", b) for b in bits_of(ways)] + [("dp", b) for b in bits_of(groups)]

    def begin(self, step):
        axis, bit = self.steps[step]
        index = self.place[1] if axis == "tensor" else self.place[0]
        source = self.values if step == 0 else self.sums.at[step - 1]
        self.copy = pltpu.make_async_remote_copy(
            src_ref=source, dst_ref=self.arrived.at[step], send_sem=self.sems[0].at[step],
            recv_sem=self.sems[1].at[step], device_id={axis: partner_of(index, bit)},
            device_id_type=pl.DeviceIdType.MESH,
        )
        self.copy.start()

    def finish(self, step):
        self.copy.wait()
        axis, bit = self.steps[step]
        source = self.values if step == 0 else self.sums.at[step - 1]
        for r in range(self.ways + 1):
            swapped = r ^ bit if axis == "tensor" and r < self.ways else r
            self.sums[step, 8 * r : 8 * r + 8, :] = (
                source[8 * r : 8 * r + 8, :] + self.arrived[step, 8 * swapped : 8 * swapped + 8, :]
            )


def backward_kernel(ways, groups, cuts, counts, *refs):
    refs = list(refs)

    def take(count):
        taken, refs[:] = refs[:count], refs[count:]
        return taken

    (length_ref,) = take(1)
    d_down, d_up = take(ways), take(ways)
    queries, keys, values, logs, contexts = [take(ways) for _ in range(5)]
    w_out, w_query, w_key, w_value = [take(ways) for _ in range(4)]
    tokens_t, d_one_low, d_one, small = take(4)
    outs = take(len(cuts))
    small_out, grad_tokens = take(2)
    d_out, d_joint = take(ways), take(ways)
    d_context, d_heads, small_own, small_sums, small_arrived = take(5)
    small_send, small_recv, chunk_send, chunk_recv = take(4)
    place = (lax.axis_index("dp"), lax.axis_index("tensor"))

    barrier = pltpu.get_barrier_semaphore()
    partners = [{"tensor": partner_of(place[1], b)} for b in bits_of(ways)]
    partners += [{"dp": partner_of(place[0], b)} for b in bits_of(groups)]
    for partner in partners:
        pl.semaphore_signal(barrier, inc=1, device_id=partner, device_id_type=pl.DeviceIdType.MESH)
    pl.semaphore_wait(barrier, len(partners))

    bits = len(bits_of(groups))
    blocks = [d_down, d_up, d_out, d_joint]
    chunks, finals = [], []
    for w, cut in enumerate(cuts):
        rows = counts[w] // cut
        for c in range(cut):
            own = [block.at[c * rows : (c + 1) * rows, :] for block in blocks[w]]
            near, far, full, *arrived = take(4 + bits)
            number = len(chunks)
            chunks.append(
                Chunk(own, near, far, full, arrived, place, (chunk_send.at[number], chunk_recv.at[number]), groups)
            )
            finals.append((outs[w], c * rows, rows))
    vectors = Vectors(small_own, small_sums, small_arrived, place, (small_send, small_recv), ways, groups)
    early = chunks[: cuts[0] + cuts[1]]
    middle = chunks[len(early) : len(early) + cuts[2]]
    late = chunks[len(early) + cuts[2] :]

    def shard(r):
        d_context[...] = dot(d_one_low[...], w_out[r][...], NT).astype(BF16)
        attend_backward(length_ref[0], queries[r], keys[r], values[r], logs[r], d_context, d_heads)
        d_joint[r][...] = jnp.dot(tokens_t[...], d_heads[...], preferred_element_type=F32).astype(BF16)
        cols = w_query[r].shape[1]
        total = grad_tokens[...]
        for third, weight in enumerate((w_query[r], w_key[r], w_value[r])):
            total = total + dot(d_heads[:, third * cols : (third + 1) * cols], weight[...], NT)
        grad_tokens[...] = total
        small_own[8 * r + 1 : 8 * r + 2, : 3 * cols] = jnp.sum(d_heads[...].astype(F32), 0, keepdims=True)

    for chunk in early:
        chunk.pair_start()
    small_own[...] = small[...]
    grad_tokens[...] = d_one[...]
    for r in (3, 1, 2, 0):
        d_out[r][...] = jnp.dot(contexts[r][...], d_one_low[...], preferred_element_type=F32).astype(BF16)
    early[0].pair_finish()
    for chunk in middle:
        chunk.pair_start()
    shard(3)
    for chunk in early[1:2]:
        chunk.pair_finish()
    shard(1)
    for chunk in late:
        chunk.pair_start()
    for chunk in early[2:]:
        chunk.pair_finish()
    early[0].finish(0)
    early[0].begin(0)
    shard(2)
    for chunk in middle:
        chunk.pair_finish()
    shard(0)
    late[0].pair_finish()
    vectors.begin(0)
    for chunk in late[1:]:
        chunk.pair_finish()
    vectors.finish(0)
    vectors.begin(1)

    last = 2 * bits
    steps = len(vectors.steps)
    first_wave = len(chunks) - 1
    for wave in range(max(len(chunks) + last, first_wave + steps)):
        if 0 <= wave - first_wave < steps - 1:
            vectors.finish(wave - first_wave + 1)
            if wave - first_wave + 2 < steps:
                vectors.begin(wave - first_wave + 2)
        for n in range(len(chunks)):
            stage = wave - n
            if not 0 <= stage <= last or (n, stage) == (0, 0):
                continue
            chunks[n].finish(stage)
            if stage < last:
                chunks[n].begin(stage)
            else:
                out, start, rows = finals[n]
                out[start : start + rows, :] = chunks[n].full[...]
    small_out[...] = small_sums[steps - 1]


def backward(length, d_down, d_up, saved, w_out, w_query, w_key, w_value, tokens_t, d_one_low, d_one, small):
    ways, groups = lax.axis_size("tensor"), lax.axis_size("dp")
    assert ways == 4
    bits = len(bits_of(groups))
    steps = bits + len(bits_of(ways))
    width, own_rows = tokens_t.shape
    cols = w_query[0].shape[1]
    shape = jax.ShapeDtypeStruct
    shapes = [d_down[0].shape, d_up[0].shape, w_out[0].shape, (width, 3 * cols)]
    cuts = (2, 2, 1, 2)
    scratch = [pltpu.VMEM(shapes[2], BF16)] * ways + [pltpu.VMEM(shapes[3], BF16)] * ways
    scratch += [
        pltpu.VMEM((own_rows, cols), BF16),
        pltpu.VMEM((own_rows, 3 * cols), BF16),
        pltpu.VMEM(small.shape, F32),
        pltpu.VMEM((steps,) + small.shape, F32),
        pltpu.VMEM((steps,) + small.shape, F32),
        pltpu.SemaphoreType.DMA((steps,)),
        pltpu.SemaphoreType.DMA((steps,)),
        pltpu.SemaphoreType.DMA((sum(cuts), 3 + 2 * bits)),
        pltpu.SemaphoreType.DMA((sum(cuts), 3 + 2 * bits)),
    ]
    for (rows, columns), cut in zip(shapes, cuts):
        for _ in range(cut):
            scratch += [pltpu.VMEM((rows // cut, columns), BF16)] * 4
            scratch += [pltpu.VMEM((count, columns), BF16) for _, count, _ in halvings(rows // cut, groups)]
    operands = list(d_down) + list(d_up)
    for item in range(5):
        operands += [kept[item] for kept in saved]
    operands += list(w_out) + list(w_query) + list(w_key) + list(w_value)
    operands += [tokens_t, d_one_low, d_one, small]
    outs = pl.pallas_call(
        functools.partial(backward_kernel, ways, groups, cuts, [s[0] for s in shapes]),
        out_shape=[shape(s, BF16) for s in shapes] + [shape(small.shape, F32), shape(d_one.shape, F32)],
        in_specs=[SMEM_SPEC] + [VMEM_SPEC] * len(operands),
        out_specs=[VMEM_SPEC] * 6,
        scratch_shapes=scratch,
        compiler_params=pltpu.CompilerParams(
            collective_id=0, has_side_effects=True, vmem_limit_bytes=67043328
        ),
        name="backward",
    )(length, *operands)
    return [o.astype(F32) for o in outs[:4]], outs[4], outs[5]


def dot(left, right, dims):
    return lax.dot_general(left, right, (dims, ((), ())), preferred_element_type=F32)


NN = ((1,), (0,))
NT = ((1,), (1,))
TN = ((0,), (0,))


def attend_forward_kernel(
    length_ref, rows_ref, wq_ref, wk_ref, wv_ref, bq_ref, bv_ref,
    q_ref, k_ref, v_ref, context_ref, context_t_ref, log_ref,
):
    length = length_ref[0]
    rows = rows_ref[...]
    q_ref[...] = (jnp.dot(rows, wq_ref[...], preferred_element_type=F32) + bq_ref[...]).astype(BF16)
    k_ref[...] = jnp.dot(rows, wk_ref[...], preferred_element_type=F32).astype(BF16)
    v_ref[...] = (jnp.dot(rows, wv_ref[...], preferred_element_type=F32) + bv_ref[...]).astype(BF16)
    size = rows.shape[0]
    key_valid = lax.broadcasted_iota(jnp.int32, (size, size), 0) < length
    for head in range(q_ref.shape[1] // HEAD_DIM):
        part = slice(head * HEAD_DIM, (head + 1) * HEAD_DIM)
        scaled = (q_ref[:, part].astype(F32) * HEAD_DIM ** (-0.5)).astype(BF16)
        scores = dot(k_ref[:, part], scaled, NT)
        scores = jnp.where(key_valid, scores, -1e30)
        highest = jnp.max(scores, 0, keepdims=True)
        expo = jnp.exp(scores - highest)
        totals = jnp.sum(expo, 0, keepdims=True)
        probs_low = (expo * (1.0 / totals)).astype(BF16)
        context_t = dot(v_ref[:, part], probs_low, TN)
        context_t_ref[part, :] = context_t.astype(BF16)
        context_ref[:, part] = context_t.T.astype(BF16)
        log_ref[head : head + 1, :] = highest + jnp.log(totals)


def attend_backward(length, q_ref, k_ref, v_ref, log_ref, d_context_ref, d_joint_ref):
    size, cols = q_ref.shape
    key_valid = lax.broadcasted_iota(jnp.int32, (size, size), 0) < length
    for head in range(cols // HEAD_DIM):
        part = slice(head * HEAD_DIM, (head + 1) * HEAD_DIM)
        scaled = (q_ref[:, part].astype(F32) * HEAD_DIM ** (-0.5)).astype(BF16)
        keys = k_ref[:, part]
        d_context = d_context_ref[:, part]
        scores = dot(keys, scaled, NT)
        scores = jnp.where(key_valid, scores, -1e30)
        probs = jnp.exp(scores - log_ref[head : head + 1, :])
        d_probs = dot(v_ref[:, part], d_context, NT)
        d_value = jnp.dot(probs.astype(BF16), d_context, preferred_element_type=F32)
        centre = jnp.sum(probs * d_probs, 0, keepdims=True)
        d_scores = (probs * (d_probs - centre)).astype(BF16)
        d_key = jnp.dot(d_scores, scaled, preferred_element_type=F32)
        d_query_t = dot(keys, d_scores, TN) * HEAD_DIM ** (-0.5)
        for third, value in enumerate((d_query_t.T, d_key, d_value)):
            start = third * cols + head * HEAD_DIM
            d_joint_ref[:, start : start + HEAD_DIM] = value.astype(BF16)


VMEM_SPEC = pl.BlockSpec(memory_space=pltpu.VMEM)
SMEM_SPEC = pl.BlockSpec(memory_space=pltpu.SMEM)


def attend_forward(length, rows, wq, wk, wv, bq, bv):
    count, cols = rows.shape[0], wq.shape[1]
    shape = jax.ShapeDtypeStruct
    heads = cols // HEAD_DIM
    return pl.pallas_call(
        attend_forward_kernel,
        out_shape=[shape((count, cols), BF16)] * 4 + [shape((cols, count), BF16), shape((heads, count), F32)],
        in_specs=[SMEM_SPEC] + [VMEM_SPEC] * 6,
        out_specs=[VMEM_SPEC] * 6,
        cost_estimate=pl.CostEstimate(
            flops=2 * count * (3 * rows.shape[1] * cols + 2 * count * cols),
            bytes_accessed=2 * (rows.size + 3 * wq.size + 5 * count * cols),
            transcendentals=count * count * heads,
        ),
        compiler_params=pltpu.CompilerParams(vmem_limit_bytes=32 * 2**20),
        name="attend_forward",
    )(length, rows, wq, wk, wv, bq, bv)


def normalise(value):
    centre = value - jnp.mean(value, -1, keepdims=True)
    inverse = lax.rsqrt(jnp.mean(centre * centre, -1, keepdims=True) + EPSILON)
    return centre * inverse, inverse


def norm_back(incoming, normal, inverse, gain):
    d_gain = jnp.sum(incoming * normal, 0)
    d_shift = jnp.sum(incoming, 0)
    scaled = incoming * gain
    d_input = inverse * (
        scaled
        - jnp.mean(scaled, -1, keepdims=True)
        - normal * jnp.mean(scaled * normal, -1, keepdims=True)
    )
    return d_input, d_gain, d_shift


def local(
    tokens, lengths, w_query, b_query, w_key, w_value, b_value, w_out, b_out,
    gain_one, shift_one, w_up, b_up, w_down, b_down, gain_two, shift_two, cotangent,
):
    own_rows, width = tokens.shape
    ways = lax.axis_size("tensor")
    me = lax.axis_index("tensor")
    local_cols = w_query.shape[1]
    length = lax.dynamic_slice(lengths, (me,), (1,))
    gain_a, shift_a = gain_one.astype(F32), shift_one.astype(F32)
    gain_b, shift_b = gain_two.astype(F32), shift_two.astype(F32)

    biases = jnp.concatenate([b_query, b_value, b_up]).reshape(1, -1).astype(F32)
    biases = gather_blocks(biases, "tensor")
    b_query_all = [b[:, :local_cols] for b in biases]
    b_value_all = [b[:, local_cols : 2 * local_cols] for b in biases]
    b_up_all = [b[:, 2 * local_cols :] for b in biases]
    wq_all = gather_blocks(w_query, "tensor")
    wk_all = gather_blocks(w_key, "tensor")
    wv_all = gather_blocks(w_value, "tensor")
    wo_all = gather_blocks(w_out, "tensor")
    up_all = gather_blocks(w_up, "tensor")
    down_all = gather_blocks(w_down, "tensor")

    saved, attn_out = [], 0.0
    for r in range(ways):
        q, k, v, context, context_t, log_total = attend_forward(
            length, tokens, wq_all[r], wk_all[r], wv_all[r], b_query_all[r], b_value_all[r]
        )
        saved.append((q, k, v, log_total, context_t))
        attn_out = attn_out + dot(context, wo_all[r], NN)
    resid_one = tokens.astype(F32) + attn_out + b_out.astype(F32)
    unit_one, inverse_one = normalise(resid_one)
    normed_one = unit_one * gain_a + shift_a
    normed_low = normed_one.astype(BF16)

    ffn_out, acts, slopes = 0.0, [], []
    for r in range(ways):
        pre_act = dot(normed_low, up_all[r], NN) + b_up_all[r]
        share = 0.5 * (1.0 + lax.erf(pre_act * 0.5**0.5))
        activ = (pre_act * share).astype(BF16)
        slope = share + pre_act * jnp.exp(-0.5 * pre_act * pre_act) * (2.0 * jnp.pi) ** (-0.5)
        acts.append(activ)
        slopes.append(slope)
        ffn_out = ffn_out + dot(activ, down_all[r], NN)
    unit_two, inverse_two = normalise(normed_one + ffn_out + b_down.astype(F32))
    result = (unit_two * gain_b + shift_b).astype(BF16)

    row_valid = (jnp.arange(own_rows) < length[0]).astype(F32)[:, None]
    incoming = cotangent.astype(F32) * row_valid
    d_two, d_gain_two, d_shift_two = norm_back(incoming, unit_two, inverse_two, gain_b)
    d_b_down = jnp.sum(d_two, 0)
    d_two_low = d_two.astype(BF16)
    d_one_out = d_two
    d_down, d_up, d_b_up = [None] * ways, [None] * ways, [None] * ways
    for r in reversed(range(ways)):
        d_down[r] = dot(acts[r], d_two_low, TN).astype(BF16)
        d_pre = (dot(d_two_low, down_all[r], NT) * slopes[r]).astype(BF16)
        d_up[r] = dot(normed_low, d_pre, TN).astype(BF16)
        d_b_up[r] = jnp.sum(d_pre.astype(F32), 0)
        d_one_out = d_one_out + dot(d_pre, up_all[r], NT)

    d_one, d_gain_one, d_shift_one = norm_back(d_one_out, unit_one, inverse_one, gain_a)
    d_b_out = jnp.sum(d_one, 0)
    d_one_low = d_one.astype(BF16)
    parts = []
    for r in range(ways):
        parts += [d_b_up[r]] + [jnp.zeros((width,), F32)] * 7
    parts += [d_gain_one, d_shift_one, d_b_out, d_b_down, d_gain_two, d_shift_two] + [jnp.zeros((width,), F32)] * 2
    sums, small, grad_tokens = backward(
        length, d_down, d_up, saved, wo_all, wq_all, wk_all, wv_all, tokens.T, d_one_low, d_one, jnp.stack(parts)
    )
    grad_w_down, grad_w_up, grad_w_out, d_w_joint = sums
    shared = small[8 * ways :]

    return (
        result,
        grad_tokens,
        d_w_joint[:, :local_cols],
        small[1, :local_cols],
        d_w_joint[:, local_cols : 2 * local_cols],
        d_w_joint[:, 2 * local_cols :],
        small[1, 2 * local_cols : 3 * local_cols],
        grad_w_out,
        shared[2],
        shared[0],
        shared[1],
        grad_w_up,
        small[0],
        grad_w_down,
        shared[3],
        shared[4],
        shared[5],
    )


def solution(mesh):
    rows = P(("dp", "tensor"), None)
    in_specs = (
        rows, P("dp"), P(None, "tensor"), P("tensor"), P(None, "tensor"), P(None, "tensor"), P("tensor"),
        P("tensor", None), P(), P(), P(), P(None, "tensor"), P("tensor"), P("tensor", None), P(), P(), P(), rows,
    )
    out_specs = (
        rows, rows, P(None, "tensor"), P("tensor"), P(None, "tensor"), P(None, "tensor"), P("tensor"),
        P("tensor", None), P(), P(), P(), P(None, "tensor"), P("tensor"), P("tensor", None), P(), P(), P(),
    )
    return jax.shard_map(local, mesh=mesh, in_specs=in_specs, out_specs=out_specs, check_vma=False)
```
